32 devices in a mesh: blk: 8 (over z, x), dp: 4 (over y, core).
Axes of the slice: x: 2, y: 2, z: 4, core: 2. Of those that a mesh axis runs over, the one named last changes fastest.
Arguments:
- embeddings: bfloat16 [8192, 512], P(('dp', 'blk')), may hold values from -16 to 16
- centers: bfloat16 [16384, 512], P(('blk', 'dp')), may hold values from -10 to 10
- labels: int32 [8192], P(('dp', 'blk')), may hold values from 0 to 16383
Outputs:
- loss: float32 [8192], P(('dp', 'blk'))
The draws below stay inside these ranges and needn't reach their ends.
All inputs are finite; a program needn't handle non-finite values.
Results may differ from the reference program's by a relative error of at most 0.0017.
Values may be sent and summed in bfloat16 or wider, within the bound.
A program may use at most 128 MiB of HBM per device.

```python
import math
import jax
import jax.numpy as jnp
from jax import lax

D = 512
BATCH = 8192
CLASSES = 16384


def label_values(key):
    return jax.random.randint(jax.random.fold_in(key, 11), (BATCH,), 0, CLASSES, dtype=jnp.int32)


def center_values(key):
    center_key = jax.random.fold_in(key, 12)
    return jax.random.truncated_normal(center_key, -6.0, 6.0, (CLASSES, D), jnp.float32)


def draw_labels(key, part):
    return label_values(key)


def draw_centers(key, part):
    return center_values(key).astype(jnp.bfloat16)


def draw_embeddings(key, part):
    labels = label_values(key)
    centers = center_values(key).astype(jnp.bfloat16).astype(jnp.float32)
    unit = centers * jax.lax.rsqrt(jnp.sum(centers * centers, axis=1, keepdims=True) + 1e-06)
    negatives = jax.random.randint(jax.random.fold_in(key, 14), (BATCH, 4), 0, CLASSES, dtype=jnp.int32)
    active_count = jax.random.randint(jax.random.fold_in(key, 15), (BATCH, 1), 2, 5, dtype=jnp.int32)
    active = (jnp.arange(4, dtype=jnp.int32)[None, :] < active_count).astype(jnp.float32)
    own_lo, own_hi, neg_lo, neg_hi = (0.6, 0.9, 0.3, 0.5)
    weights = jax.random.uniform(jax.random.fold_in(key, 16), (BATCH, 4), jnp.float32, neg_lo, neg_hi) * active
    own = jax.random.uniform(jax.random.fold_in(key, 17), (BATCH, 1), jnp.float32, own_lo, own_hi)
    mixed = own * unit[labels]
    for slot in range(4):
        mixed = mixed + weights[:, slot:slot + 1] * unit[negatives[:, slot]]
    noise_key = jax.random.fold_in(key, 18)
    noise = jax.random.normal(noise_key, (BATCH, D), jnp.float32)
    values = math.sqrt(D) * (mixed + 0.3 * noise / math.sqrt(D))
    return jnp.clip(values, -16.0, 16.0).astype(jnp.bfloat16)


def setup_inputs(seed: int = 0) -> dict:
    keys = jax.random.split(jax.random.key(seed), 4)
    return {
        "embeddings": draw_embeddings(jax.random.fold_in(keys[3], 71), 0),
        "centers": draw_centers(jax.random.fold_in(keys[3], 71), 0),
        "labels": draw_labels(jax.random.fold_in(keys[3], 71), 0),
    }


EPSILON = 1e-06
LOGIT_SCALE = 30.0
MARGIN = 0.5

def unit_rows(matrix):
    values = matrix.astype(jnp.float32)
    return (values * lax.rsqrt(lax.optimization_barrier(jnp.sum(values * values, axis=1, keepdims=True)) + EPSILON)).astype(jnp.bfloat16)

def margin_loss(other_sum, target_cos):
    sine = jnp.sqrt(jnp.maximum(1.0 - target_cos * target_cos, 0.0))
    shifted = target_cos * math.cos(MARGIN) - sine * math.sin(MARGIN)
    return LOGIT_SCALE + jnp.log(other_sum + jnp.exp(LOGIT_SCALE * shifted - LOGIT_SCALE)) - LOGIT_SCALE * shifted

def block_terms(rows, row_labels, centers_block):
    cosine = jnp.dot(rows, centers_block.T, preferred_element_type=jnp.float32)
    columns = jnp.arange(centers_block.shape[0], dtype=jnp.int32)
    is_target = row_labels[:, None] == columns[None, :]
    other_sum = lax.optimization_barrier(jnp.sum(jnp.where(is_target, 0.0, jnp.exp(LOGIT_SCALE * cosine - LOGIT_SCALE)), axis=1))
    target_cos = lax.optimization_barrier(jnp.sum(jnp.where(is_target, cosine, 0.0), axis=1))
    return (other_sum, target_cos)

def reference(embeddings, centers, labels):
    emb_unit = unit_rows(embeddings)
    center_unit = unit_rows(centers)
    span_rows = math.gcd(BATCH, 1024)
    emb_blocks = emb_unit.reshape(-1, span_rows, D)
    label_blocks = labels.reshape(-1, span_rows)

    def one_block(pair):
        return block_terms(pair[0], pair[1], center_unit)
    other_sum, target_cos = lax.map(one_block, (emb_blocks, label_blocks))
    return margin_loss(other_sum.reshape(-1), target_cos.reshape(-1))
```

```python
import functools
import math

import jax
import jax.numpy as jnp
from jax import lax
from jax.experimental import pallas as pl
from jax.experimental.pallas import tpu as pltpu
from jax.sharding import PartitionSpec as P

EPSILON = 1e-06
LOGIT_SCALE = 30.0
MARGIN = 0.5
MESH = pl.DeviceIdType.MESH


def unit_rows(matrix):
    values = matrix.astype(jnp.float32)
    return (values * lax.rsqrt(jnp.sum(values * values, axis=1, keepdims=True) + EPSILON)).astype(
        jnp.bfloat16
    )


def margin_loss(other_sum, target_cos):
    sine = jnp.sqrt(jnp.maximum(1.0 - target_cos * target_cos, 0.0))
    shifted = target_cos * math.cos(MARGIN) - sine * math.sin(MARGIN)
    return (
        LOGIT_SCALE
        + jnp.log(other_sum + jnp.exp(LOGIT_SCALE * shifted - LOGIT_SCALE))
        - LOGIT_SCALE * shifted
    )


def kernel(
    depth,
    emb_ref,
    cen_ref,
    lab_ref,
    out_ref,
    emb_raw,
    sib_raw,
    cen_raw,
    emb_n,
    cen_n,
    labels,
    acc_o,
    acc_t,
    part,
    parts_in,
    bases,
    local_sem,
    lab_send,
    lab_recv,
    row_recv,
    up_send,
    down_send,
    sib_send,
    sib_recv,
    x_send,
    x_recv,
    y_send,
    y_recv,
    part_send,
    part_recv,
):
    blk, dp = lax.axis_index("blk"), lax.axis_index("dp")
    z, x = blk // 2, blk % 2
    y, core = dp // 2, dp % 2
    rows, width = emb_raw.shape[2:]
    quarter = cen_raw.shape[2]
    group = 2 * depth
    here = 2 * z + core
    center_tiles = cen_raw.shape[0]
    center_rounds = center_tiles - 2
    row_rounds = 2 * (depth - 1)
    rounds = max(center_rounds, row_rounds)

    def device(zz, xx, yy, cc):
        return {"blk": 2 * zz + xx, "dp": 2 * yy + cc}

    def member_at(j):
        return lax.rem(z + j // 2, depth), (core + j) % 2

    def member(j):
        zz, cc = member_at(j)
        return device(zz, x, y, cc)

    x_peer = device(z, 1 - x, y, core)
    y_peer = device(z, x, 1 - y, core)
    sibling = device(z, x, y, 1 - core)
    above = device(jnp.minimum(z + 1, depth - 1), x, y, core)
    below = device(jnp.maximum(z - 1, 0), x, y, core)

    def remote(src, dst, send, recv, to):
        return pltpu.make_async_remote_copy(
            src_ref=src, dst_ref=dst, send_sem=send, recv_sem=recv, device_id=to, device_id_type=MESH
        )

    local = [
        pltpu.make_async_copy(cen_ref, cen_raw.at[pl.ds(0, 2)], local_sem.at[0]),
        pltpu.make_async_copy(emb_ref, emb_raw.at[z], local_sem.at[1]),
        pltpu.make_async_copy(lab_ref, labels.at[z, core], local_sem.at[2]),
    ]
    for copy in local:
        copy.start()

    barrier = pltpu.get_barrier_semaphore()
    for j in range(1, group):
        pl.semaphore_signal(barrier, inc=1, device_id=member(j), device_id_type=MESH)
    for to in (x_peer, y_peer):
        pl.semaphore_signal(barrier, inc=1, device_id=to, device_id_type=MESH)

    def block_start(xx, yy):
        return ((2 * z + xx) * 4 + 2 * yy + core) * (4 * quarter)

    own = block_start(x, y)
    from_x, from_y, from_xy = block_start(1 - x, y), block_start(x, 1 - y), block_start(1 - x, 1 - y)
    starts = [own, own + quarter, own + 2 * quarter, own + 3 * quarter]
    for first, second in zip(range(4), (2, 3, 0, 1)):
        starts += [from_x + first * quarter, from_y + second * quarter]
    for first, second in ((2, 0), (3, 1)):
        starts += [from_xy + first * quarter, from_xy + second * quarter]
    for i, start in enumerate(starts):
        bases[i] = start
    acc_o[...] = jnp.zeros_like(acc_o)
    acc_t[...] = jnp.zeros_like(acc_t)

    for copy in local:
        copy.wait()
    pl.semaphore_wait(barrier, group + 1)

    def row_copy(g, sems, to):
        ref = emb_raw.at[g // 2, g % 2]
        return remote(ref, ref, sems.at[g], row_recv.at[g], to)

    def sib_copy(g):
        return remote(
            emb_raw.at[g // 2, g % 2], sib_raw.at[g // 2, g % 2], sib_send.at[g], sib_recv.at[g], sibling
        )

    def x_copy(t, tile, side):
        return remote(cen_raw.at[tile, side], cen_raw.at[t + 1, 0], x_send.at[t], x_recv.at[t], x_peer)

    def y_copy(t, tile, side):
        return remote(cen_raw.at[tile, side], cen_raw.at[t + 1, 1], y_send.at[t], y_recv.at[t], y_peer)

    def lab_copy(j):
        ref = labels.at[z, core]
        return remote(ref, ref, lab_send.at[j], lab_recv.at[j], member(j))

    up_ok, down_ok = z + 1 < depth, z > 0

    def send_up(g):
        @pl.when(up_ok)
        def _():
            row_copy(g, up_send, above).start()

    def send_down(g):
        @pl.when(down_ok)
        def _():
            row_copy(g, down_send, below).start()

    for j in range(1, group):
        lab_copy(j).start()
    send_up(2 * z + 1)
    send_down(2 * z)
    x_copy(1, 0, 0).start()
    y_copy(1, 1, 0).start()
    sib_copy(2 * z).start()
    sib_copy(2 * z + 1).start()
    send_up(2 * z)
    send_down(2 * z + 1)
    x_copy(2, 0, 1).start()
    y_copy(2, 1, 1).start()
    x_copy(3, 1, 0).start()
    y_copy(3, 0, 0).start()
    x_copy(4, 1, 1).start()
    y_copy(4, 0, 1).start()

    def ready_rows(g):
        emb_n[g, core] = unit_rows(emb_raw[g // 2, g % 2])

    def ready_sib(g):
        emb_n[g, 1 - core] = unit_rows(sib_raw[g // 2, g % 2])

    def ready_center(r):
        for side in range(2):
            cen_n[r, side] = unit_rows(cen_raw[r, side])

    def pair(g, r):
        cosine = lax.dot_general(
            cen_n[r].reshape(2 * quarter, width),
            emb_n[g].reshape(2 * rows, width),
            (((1,), (1,)), ((), ())),
            preferred_element_type=jnp.float32,
        )
        label = jnp.concatenate([labels[g // 2, 0, g % 2], labels[g // 2, 1, g % 2]], axis=1)
        index = lax.broadcasted_iota(jnp.int32, (quarter, 2 * rows), 0)
        others, targets = acc_o[g], acc_t[g]
        for side in range(2):
            cos = cosine[side * quarter : (side + 1) * quarter]
            hit = index == label - bases[2 * r + side]
            power = jnp.where(hit, 0.0, jnp.exp2(cos * (LOGIT_SCALE * math.log2(math.e))))
            others += jnp.sum(power.reshape(-1, 8, 2 * rows), axis=0)
            targets += jnp.sum(jnp.where(hit, cos, 0.0).reshape(-1, 8, 2 * rows), axis=0)
        acc_o[g] = others
        acc_t[g] = targets

    def pairs(g_lo, g_hi, r_lo, r_hi):
        @pl.loop(g_lo, g_hi)
        def _(g):
            @pl.loop(r_lo, r_hi)
            def _(r):
                pair(g, r)

    for h in range(2):
        ready_rows(2 * z + h)
        ready_center(h)
    for h in range(2):
        sib_copy(2 * z + h).wait_recv()
        ready_sib(2 * z + h)
    lab_copy(1).wait_recv()
    pairs(2 * z, 2 * z + 2, 0, 2)
    for j in range(2, group):
        lab_copy(j).wait_recv()

    def one_round(t, ignored):
        low, high = 2 * z - t, 2 * z + 1 + t
        has_low, has_high = low >= 0, high < group

        @pl.when(has_low)
        def _():
            row_copy(low, up_send, above).wait_recv()
            sib_copy(low).start()

            @pl.when(up_ok)
            def _():
                row_copy(low, up_send, above).start()

        @pl.when(has_high)
        def _():
            row_copy(high, down_send, below).wait_recv()
            sib_copy(high).start()

            @pl.when(down_ok)
            def _():
                row_copy(high, down_send, below).start()

        @pl.when(t <= center_rounds)
        def _():
            x_copy(t, 0, 0).wait_recv()
            y_copy(t, 0, 0).wait_recv()

        @pl.when(t <= center_rounds - 4)
        def _():
            x_copy(t + 4, t + 1, 1).start()
            y_copy(t + 4, t + 1, 0).start()

        done = jnp.minimum(t, center_rounds) + 1
        g_lo, g_hi = jnp.maximum(low + 1, 0), jnp.minimum(high, group)

        @pl.when(t <= center_rounds)
        def _():
            ready_center(t + 1)

        @pl.when(has_low)
        def _():
            ready_rows(low)

        @pl.when(has_high)
        def _():
            ready_rows(high)

        pairs(g_lo, g_hi, done, jnp.minimum(t + 1, center_rounds + 1) + jnp.where(t <= center_rounds, 1, 0))

        @pl.when(has_low)
        def _():
            sib_copy(low).wait_recv()
            ready_sib(low)

        @pl.when(has_high)
        def _():
            sib_copy(high).wait_recv()
            ready_sib(high)

        last = jnp.minimum(t, center_rounds) + 2
        pairs(low, jnp.where(has_low, low + 1, low), 0, last)
        pairs(high, jnp.where(has_high, high + 1, high), 0, last)
        return ignored

    lax.fori_loop(1, rounds + 1, one_round, 0)

    for g in range(group):
        for quantity, acc in enumerate((acc_o, acc_t)):
            total = jnp.sum(acc[g], axis=0, keepdims=True)
            for cc in range(2):
                part[2 * (g // 2) + cc, quantity, g % 2] = total[:, cc * rows : (cc + 1) * rows]

    def part_copy(j):
        zz, cc = member_at(j)
        return remote(
            part.at[2 * zz + cc], parts_in.at[j], part_send.at[j], part_recv.at[j], member(j)
        )

    for j in range(1, group):
        part_copy(j).start()
    other_sum, target_cos = part[here, 0], part[here, 1]
    for j in range(1, group):
        part_copy(j).wait_recv()
        other_sum += parts_in[j, 0]
        target_cos += parts_in[j, 1]
    out_ref[...] = margin_loss(other_sum * math.exp(-LOGIT_SCALE), target_cos)

    for j in range(1, group):
        lab_copy(j).wait_send()
        part_copy(j).wait_send()
    for t in range(1, center_rounds + 1):
        x_copy(t, 0, 0).wait_send()
        y_copy(t, 0, 0).wait_send()

    @pl.loop(0, group)
    def _(g):
        sib_copy(g).wait_send()

        @pl.when(up_ok & (g < 2 * z + 2))
        def _():
            row_copy(g, up_send, above).wait_send()

        @pl.when(down_ok & (g >= 2 * z))
        def _():
            row_copy(g, down_send, below).wait_send()


def body(depth, embeddings, centers, labels):
    count, width = embeddings.shape
    classes = centers.shape[0]
    rows, quarter, group, tiles = count // 2, classes // 4, 2 * depth, 8
    any_spec = pl.BlockSpec(memory_space=pl.ANY)
    dma = pltpu.SemaphoreType.DMA
    loss = pl.pallas_call(
        functools.partial(kernel, depth),
        out_shape=jax.ShapeDtypeStruct((2, 1, rows), jnp.float32),
        in_specs=[any_spec] * 3,
        out_specs=pl.BlockSpec(memory_space=pltpu.VMEM),
        scratch_shapes=[
            pltpu.VMEM((depth, 2, rows, width), jnp.bfloat16),
            pltpu.VMEM((depth, 2, rows, width), jnp.bfloat16),
            pltpu.VMEM((tiles, 2, quarter, width), jnp.bfloat16),
            pltpu.VMEM((group, 2, rows, width), jnp.bfloat16),
            pltpu.VMEM((tiles, 2, quarter, width), jnp.bfloat16),
            pltpu.VMEM((depth, 2, 2, 1, rows), jnp.int32),
            pltpu.VMEM((group, 8, 2 * rows), jnp.float32),
            pltpu.VMEM((group, 8, 2 * rows), jnp.float32),
            pltpu.VMEM((group, 2, 2, 1, rows), jnp.float32),
            pltpu.VMEM((group, 2, 2, 1, rows), jnp.float32),
            pltpu.SMEM((2 * tiles,), jnp.int32),
            dma((3,)),
            dma((group,)),
            dma((group,)),
            dma((group,)),
            dma((group,)),
            dma((group,)),
            dma((group,)),
            dma((group,)),
            dma((tiles,)),
            dma((tiles,)),
            dma((tiles,)),
            dma((tiles,)),
            dma((group,)),
            dma((group,)),
        ],
        compiler_params=pltpu.CompilerParams(
            collective_id=0, has_side_effects=True, vmem_limit_bytes=48 * 1024 * 1024
        ),
    )(
        embeddings.reshape(2, rows, width),
        centers.reshape(2, 2, quarter, width),
        labels.reshape(2, 1, rows),
    )
    return loss.reshape(-1)


def solution(mesh):
    return jax.shard_map(
        functools.partial(body, mesh.shape["blk"] // 2),
        mesh=mesh,
        in_specs=(P(("dp", "blk"), None), P(("blk", "dp"), None), P(("dp", "blk"))),
        out_specs=P(("dp", "blk")),
        check_vma=False,
    )
```

```python
import functools
import math

import jax
import jax.numpy as jnp
from jax import lax
from jax.experimental import pallas as pl
from jax.experimental.pallas import tpu as pltpu
from jax.sharding import PartitionSpec as P

EPSILON = 1e-06
LOGIT_SCALE = 30.0
MARGIN = 0.5
MESH = pl.DeviceIdType.MESH


def unit_rows(matrix):
    values = matrix.astype(jnp.float32)
    return (values * lax.rsqrt(jnp.sum(values * values, axis=1, keepdims=True) + EPSILON)).astype(
        jnp.bfloat16
    )


def margin_loss(other_sum, target_cos):
    sine = jnp.sqrt(jnp.maximum(1.0 - target_cos * target_cos, 0.0))
    shifted = target_cos * math.cos(MARGIN) - sine * math.sin(MARGIN)
    return (
        LOGIT_SCALE
        + jnp.log(other_sum + jnp.exp(LOGIT_SCALE * shifted - LOGIT_SCALE))
        - LOGIT_SCALE * shifted
    )


def kernel(
    depth,
    emb_ref,
    cen_ref,
    lab_ref,
    out_ref,
    emb_raw,
    sib_raw,
    cen_raw,
    emb_n,
    cen_n,
    labels,
    acc_o,
    acc_t,
    part,
    parts_in,
    bases,
    local_sem,
    lab_send,
    lab_recv,
    row_send,
    row_recv,
    x_send,
    x_recv,
    y_send,
    y_recv,
    part_send,
    part_recv,
):
    blk, dp = lax.axis_index("blk"), lax.axis_index("dp")
    z, x = blk // 2, blk % 2
    y, core = dp // 2, dp % 2
    rows, width = emb_raw.shape[2:]
    quarter = cen_raw.shape[2]
    group = 2 * depth
    here = 2 * z + core
    center_tiles = cen_raw.shape[0]
    center_rounds = center_tiles - 2
    row_rounds = 2 * (depth - 1)
    rounds = max(center_rounds, row_rounds)

    def device(zz, xx, yy, cc):
        return {"blk": 2 * zz + xx, "dp": 2 * yy + cc}

    def member_at(j):
        return lax.rem(z + j // 2, depth), (core + j) % 2

    def member(j):
        zz, cc = member_at(j)
        return device(zz, x, y, cc)

    x_peer = device(z, 1 - x, y, core)
    y_peer = device(z, x, 1 - y, core)
    sibling = device(z, x, y, 1 - core)
    above = device(jnp.minimum(z + 1, depth - 1), x, y, core)
    below = device(jnp.maximum(z - 1, 0), x, y, core)

    def remote(src, dst, send, recv, to):
        return pltpu.make_async_remote_copy(
            src_ref=src, dst_ref=dst, send_sem=send, recv_sem=recv, device_id=to, device_id_type=MESH
        )

    local = [
        pltpu.make_async_copy(cen_ref, cen_raw.at[pl.ds(0, 2)], local_sem.at[0]),
        pltpu.make_async_copy(emb_ref, emb_raw.at[z], local_sem.at[1]),
        pltpu.make_async_copy(lab_ref, labels.at[z, core], local_sem.at[2]),
    ]
    for copy in local:
        copy.start()

    up_ok, down_ok = z + 1 < depth, z > 0
    barrier = pltpu.get_barrier_semaphore()
    for to in (sibling, x_peer, y_peer):
        pl.semaphore_signal(barrier, inc=1, device_id=to, device_id_type=MESH)

    @pl.when(up_ok)
    def _():
        pl.semaphore_signal(barrier, inc=1, device_id=above, device_id_type=MESH)

    @pl.when(down_ok)
    def _():
        pl.semaphore_signal(barrier, inc=1, device_id=below, device_id_type=MESH)

    def block_start(xx, yy):
        return ((2 * z + xx) * 4 + 2 * yy + core) * (4 * quarter)

    own = block_start(x, y)
    from_x, from_y, from_xy = block_start(1 - x, y), block_start(x, 1 - y), block_start(1 - x, 1 - y)
    starts = [own, own + quarter, own + 2 * quarter, own + 3 * quarter]
    for first, second in zip(range(4), (2, 3, 0, 1)):
        starts += [from_x + first * quarter, from_y + second * quarter]
    for first, second in ((2, 0), (3, 1)):
        starts += [from_xy + first * quarter, from_xy + second * quarter]
    for i, start in enumerate(starts):
        bases[i] = start
    acc_o[...] = jnp.zeros_like(acc_o)
    acc_t[...] = jnp.zeros_like(acc_t)

    for copy in local:
        copy.wait()
    pl.semaphore_wait(barrier, 3 + jnp.where(up_ok, 1, 0) + jnp.where(down_ok, 1, 0))

    class Pair:
        def __init__(self, *copies):
            self.copies = copies

        def start(self):
            for copy in self.copies:
                copy.start()

        def wait_recv(self):
            for copy in self.copies:
                copy.wait_recv()

        def wait_send(self):
            for copy in self.copies:
                copy.wait_send()

    def row_copy(g, way, to):
        ref, tags = emb_raw.at[g // 2, g % 2], labels.at[g // 2, core, g % 2]
        return Pair(
            remote(tags, tags, lab_send.at[way, g], lab_recv.at[0, g], to),
            remote(ref, ref, row_send.at[way, g], row_recv.at[0, g], to),
        )

    def sib_copy(g):
        tags = labels.at[g // 2, core, g % 2]
        return Pair(
            remote(tags, tags, lab_send.at[2, g], lab_recv.at[1, g], sibling),
            remote(
                emb_raw.at[g // 2, g % 2],
                sib_raw.at[g // 2, g % 2],
                row_send.at[2, g],
                row_recv.at[1, g],
                sibling,
            ),
        )

    def up_copy(g):
        return row_copy(g, 0, above)

    def down_copy(g):
        return row_copy(g, 1, below)

    def x_copy(t, tile, side):
        return remote(cen_raw.at[tile, side], cen_raw.at[t + 1, 0], x_send.at[t], x_recv.at[t], x_peer)

    def y_copy(t, tile, side):
        return remote(cen_raw.at[tile, side], cen_raw.at[t + 1, 1], y_send.at[t], y_recv.at[t], y_peer)

    def part_copy(j):
        zz, cc = member_at(j)
        return remote(
            part.at[2 * zz + cc], parts_in.at[j], part_send.at[j], part_recv.at[j], member(j)
        )

    def send_up(g):
        pl.when(up_ok)(lambda: up_copy(g).start())

    def send_down(g):
        pl.when(down_ok)(lambda: down_copy(g).start())

    send_up(2 * z + 1)
    send_down(2 * z)
    x_copy(1, 0, 0).start()
    y_copy(1, 1, 0).start()
    sib_copy(2 * z).start()
    sib_copy(2 * z + 1).start()
    send_up(2 * z)
    send_down(2 * z + 1)
    x_copy(2, 0, 1).start()
    y_copy(2, 1, 1).start()
    x_copy(3, 1, 0).start()
    y_copy(3, 0, 0).start()
    x_copy(4, 1, 1).start()
    y_copy(4, 0, 1).start()

    def ready_rows(g):
        emb_n[g, core] = unit_rows(emb_raw[g // 2, g % 2])

    def ready_sib(g):
        emb_n[g, 1 - core] = unit_rows(sib_raw[g // 2, g % 2])

    def ready_center(r):
        for side in range(2):
            cen_n[r, side] = unit_rows(cen_raw[r, side])

    def add_terms(g, first, last, others, targets):
        cosine = lax.dot_general(
            cen_n[first:last].reshape(-1, width),
            emb_n[g].reshape(2 * rows, width),
            (((1,), (1,)), ((), ())),
            preferred_element_type=jnp.float32,
        )
        label = jnp.concatenate([labels[g // 2, 0, g % 2], labels[g // 2, 1, g % 2]], axis=1)
        label = label - lax.broadcasted_iota(jnp.int32, (8, 2 * rows), 0)
        for m in range(2 * (last - first)):
            local = label - bases[2 * first + m]
            for q in range(0, quarter, 8):
                cos = cosine[m * quarter + q : m * quarter + q + 8]
                hit = local == q
                power = jnp.exp2(cos * (LOGIT_SCALE * math.log2(math.e)))
                others = others + jnp.where(hit, 0.0, power)
                targets = jnp.where(hit, cos, targets)
        return others, targets

    def pair(g, first, last):
        acc_o[g], acc_t[g] = add_terms(g, first, last, acc_o[g], acc_t[g])

    def blocks(lo, hi, first, last):
        @pl.loop(lo, hi)
        def _(zz):
            pair(2 * zz, first, last)
            pair(2 * zz + 1, first, last)

    for h in range(2):
        ready_rows(2 * z + h)
        ready_center(h)
    for h in range(2):
        sib_copy(2 * z + h).wait_recv()
        ready_sib(2 * z + h)
    blocks(z, z + 1, 0, 2)

    def receive_rows(t):
        low, high = 2 * z - t, 2 * z + 1 + t
        has_low, has_high = low >= 0, high < group

        @pl.when(has_low)
        def _():
            up_copy(low).wait_recv()
            sib_copy(low).start()
            send_up(low)

        @pl.when(has_high)
        def _():
            down_copy(high).wait_recv()
            sib_copy(high).start()
            send_down(high)

    def receive_centers(t):
        x_copy(t, 0, 0).wait_recv()
        y_copy(t, 0, 0).wait_recv()
        if t <= center_rounds - 4:
            x_copy(t + 4, t + 1, 1).start()
            y_copy(t + 4, t + 1, 0).start()

    def use_rows(t, tiles):
        low, high = 2 * z - t, 2 * z + 1 + t
        count = jnp.where(low >= 0, 1, 0) + jnp.where(high < group, 1, 0)

        @pl.loop(0, count)
        def _(i):
            g = jnp.where((low >= 0) & (i == 0), low, high)
            ready_rows(g)
            sib_copy(g).wait_recv()
            ready_sib(g)
            pair(g, 0, tiles)

    def span(t):
        return jnp.maximum(z - t // 2, 0), jnp.minimum(z + 1 + t // 2, depth)

    tiles = 2
    for t in range(1, min(rounds, center_rounds + 1)):
        receive_rows(t)
        receive_centers(t)
        ready_center(t + 1)
        if t == center_rounds - 1:
            blocks(*span(t - 1), tiles, t + 2)
            tiles = t + 2
        use_rows(t, tiles)
        if t % 2 == 0 and t < center_rounds:
            blocks(*span(t), tiles, t + 2)
            tiles = t + 2
    if rounds > center_rounds:

        @pl.loop(center_rounds + 1, rounds)
        def _(t):
            receive_rows(t)
            use_rows(t, tiles)

    receive_rows(rounds)
    if rounds == center_rounds:
        receive_centers(rounds)
        ready_center(rounds + 1)

    @pl.loop(0, depth)
    def _(i):
        zz = jnp.where(2 * z < depth, i, depth - 1 - i)

        @pl.when(i == depth - 1)
        def _():
            use_rows(rounds, tiles)

        for h in range(2):
            g = 2 * zz + h
            sums = add_terms(g, tiles, center_tiles, acc_o[g], acc_t[g])
            for quantity, total in enumerate(sums):
                total = jnp.sum(total, axis=0, keepdims=True)
                for cc in range(2):
                    part[2 * zz + cc, quantity, h] = total[:, cc * rows : (cc + 1) * rows]

        step = lax.rem(zz + depth - z, depth)

        @pl.when(step > 0)
        def _():
            part_copy(2 * step).start()

        part_copy(2 * step + 1).start()

    other_sum, target_cos = part[here, 0], part[here, 1]
    for j in range(1, group):
        part_copy(j).wait_recv()
        other_sum += parts_in[j, 0]
        target_cos += parts_in[j, 1]
    out_ref[...] = margin_loss(other_sum * math.exp(-LOGIT_SCALE), target_cos)

    for j in range(1, group):
        part_copy(j).wait_send()
    for t in range(1, center_rounds + 1):
        x_copy(t, 0, 0).wait_send()
        y_copy(t, 0, 0).wait_send()

    @pl.loop(0, group)
    def _(g):
        sib_copy(g).wait_send()
        pl.when(up_ok & (g < 2 * z + 2))(lambda: up_copy(g).wait_send())
        pl.when(down_ok & (g >= 2 * z))(lambda: down_copy(g).wait_send())


def body(depth, embeddings, centers, labels):
    count, width = embeddings.shape
    classes = centers.shape[0]
    rows, quarter, group, tiles = count // 2, classes // 4, 2 * depth, 8
    any_spec = pl.BlockSpec(memory_space=pl.ANY)
    dma = pltpu.SemaphoreType.DMA
    loss = pl.pallas_call(
        functools.partial(kernel, depth),
        out_shape=jax.ShapeDtypeStruct((2, 1, rows), jnp.float32),
        in_specs=[any_spec] * 3,
        out_specs=pl.BlockSpec(memory_space=pltpu.VMEM),
        scratch_shapes=[
            pltpu.VMEM((depth, 2, rows, width), jnp.bfloat16),
            pltpu.VMEM((depth, 2, rows, width), jnp.bfloat16),
            pltpu.VMEM((tiles, 2, quarter, width), jnp.bfloat16),
            pltpu.VMEM((group, 2, rows, width), jnp.bfloat16),
            pltpu.VMEM((tiles, 2, quarter, width), jnp.bfloat16),
            pltpu.VMEM((depth, 2, 2, 1, rows), jnp.int32),
            pltpu.VMEM((group, 8, 2 * rows), jnp.float32),
            pltpu.VMEM((group, 8, 2 * rows), jnp.float32),
            pltpu.VMEM((group, 2, 2, 1, rows), jnp.float32),
            pltpu.VMEM((group, 2, 2, 1, rows), jnp.float32),
            pltpu.SMEM((2 * tiles,), jnp.int32),
            dma((3,)),
            dma((3, group)),
            dma((2, group)),
            dma((3, group)),
            dma((2, group)),
            dma((tiles,)),
            dma((tiles,)),
            dma((tiles,)),
            dma((tiles,)),
            dma((group,)),
            dma((group,)),
        ],
        compiler_params=pltpu.CompilerParams(
            collective_id=0, has_side_effects=True, vmem_limit_bytes=48 * 1024 * 1024
        ),
    )(
        embeddings.reshape(2, rows, width),
        centers.reshape(2, 2, quarter, width),
        labels.reshape(2, 1, rows),
    )
    return loss.reshape(-1)


def solution(mesh):
    return jax.shard_map(
        functools.partial(body, mesh.shape["blk"] // 2),
        mesh=mesh,
        in_specs=(P(("dp", "blk"), None), P(("blk", "dp"), None), P(("dp", "blk"))),
        out_specs=P(("dp", "blk")),
        check_vma=False,
    )
```

```python
import functools
import math

import jax
import jax.numpy as jnp
from jax import lax
from jax.experimental import pallas as pl
from jax.experimental.pallas import tpu as pltpu
from jax.sharding import PartitionSpec as P

EPSILON = 1e-06
LOGIT_SCALE = 30.0
MARGIN = 0.5
MESH = pl.DeviceIdType.MESH


def unit_rows(matrix):
    values = matrix.astype(jnp.float32)
    return (values * lax.rsqrt(jnp.sum(values * values, axis=1, keepdims=True) + EPSILON)).astype(
        jnp.bfloat16
    )


def margin_loss(other_sum, target_cos):
    sine = jnp.sqrt(jnp.maximum(1.0 - target_cos * target_cos, 0.0))
    shifted = target_cos * math.cos(MARGIN) - sine * math.sin(MARGIN)
    return (
        LOGIT_SCALE
        + jnp.log(other_sum + jnp.exp(LOGIT_SCALE * shifted - LOGIT_SCALE))
        - LOGIT_SCALE * shifted
    )


def kernel(
    depth,
    emb_ref,
    cen_ref,
    lab_ref,
    out_ref,
    emb_raw,
    sib_raw,
    cen_raw,
    emb_n,
    cen_n,
    labels,
    acc_o,
    acc_t,
    part,
    parts_in,
    bases,
    local_sem,
    lab_send,
    lab_recv,
    row_send,
    row_recv,
    x_send,
    x_recv,
    y_send,
    y_recv,
    part_send,
    part_recv,
):
    blk, dp = lax.axis_index("blk"), lax.axis_index("dp")
    z, x = blk // 2, blk % 2
    y, core = dp // 2, dp % 2
    rows, width = emb_raw.shape[2:]
    quarter = cen_raw.shape[2]
    group = 2 * depth
    here = 2 * z + core
    center_tiles = cen_raw.shape[0]
    center_rounds = center_tiles - 2
    row_rounds = 2 * (depth - 1)
    rounds = max(center_rounds, row_rounds)

    def device(zz, xx, yy, cc):
        return {"blk": 2 * zz + xx, "dp": 2 * yy + cc}

    def member_at(j):
        return lax.rem(z + j // 2, depth), (core + j) % 2

    def member(j):
        zz, cc = member_at(j)
        return device(zz, x, y, cc)

    x_peer = device(z, 1 - x, y, core)
    y_peer = device(z, x, 1 - y, core)
    sibling = device(z, x, y, 1 - core)
    above = device(jnp.minimum(z + 1, depth - 1), x, y, core)
    below = device(jnp.maximum(z - 1, 0), x, y, core)

    def remote(src, dst, send, recv, to):
        return pltpu.make_async_remote_copy(
            src_ref=src, dst_ref=dst, send_sem=send, recv_sem=recv, device_id=to, device_id_type=MESH
        )

    local = [
        pltpu.make_async_copy(cen_ref, cen_raw.at[pl.ds(0, 2)], local_sem.at[0]),
        pltpu.make_async_copy(emb_ref, emb_raw.at[z], local_sem.at[1]),
        pltpu.make_async_copy(lab_ref, labels.at[z, core], local_sem.at[2]),
    ]
    for copy in local:
        copy.start()

    up_ok, down_ok = z + 1 < depth, z > 0
    barrier = pltpu.get_barrier_semaphore()
    for to in (sibling, x_peer, y_peer):
        pl.semaphore_signal(barrier, inc=1, device_id=to, device_id_type=MESH)

    @pl.when(up_ok)
    def _():
        pl.semaphore_signal(barrier, inc=1, device_id=above, device_id_type=MESH)

    @pl.when(down_ok)
    def _():
        pl.semaphore_signal(barrier, inc=1, device_id=below, device_id_type=MESH)

    def block_start(xx, yy):
        return ((2 * z + xx) * 4 + 2 * yy + core) * (4 * quarter)

    own = block_start(x, y)
    from_x, from_y, from_xy = block_start(1 - x, y), block_start(x, 1 - y), block_start(1 - x, 1 - y)
    starts = [own, own + quarter, own + 2 * quarter, own + 3 * quarter]
    for first, second in zip(range(4), (2, 3, 0, 1)):
        starts += [from_x + first * quarter, from_y + second * quarter]
    for first, second in ((2, 0), (3, 1)):
        starts += [from_xy + first * quarter, from_xy + second * quarter]
    for i, start in enumerate(starts):
        bases[i] = start
    acc_o[...] = jnp.zeros_like(acc_o)
    acc_t[...] = jnp.zeros_like(acc_t)

    for copy in local:
        copy.wait()
    pl.semaphore_wait(barrier, 3 + jnp.where(up_ok, 1, 0) + jnp.where(down_ok, 1, 0))

    class Pair:
        def __init__(self, *copies):
            self.copies = copies

        def start(self):
            for copy in self.copies:
                copy.start()

        def wait_recv(self):
            for copy in self.copies:
                copy.wait_recv()

        def wait_send(self):
            for copy in self.copies:
                copy.wait_send()

    def row_copy(g, way, to):
        ref, tags = emb_raw.at[g // 2, g % 2], labels.at[g // 2, core, g % 2]
        return Pair(
            remote(tags, tags, lab_send.at[way, g], lab_recv.at[0, g], to),
            remote(ref, ref, row_send.at[way, g], row_recv.at[0, g], to),
        )

    def sib_copy(g):
        tags = labels.at[g // 2, core, g % 2]
        return Pair(
            remote(tags, tags, lab_send.at[2, g], lab_recv.at[1, g], sibling),
            remote(
                emb_raw.at[g // 2, g % 2],
                sib_raw.at[g // 2, g % 2],
                row_send.at[2, g],
                row_recv.at[1, g],
                sibling,
            ),
        )

    def up_copy(g):
        return row_copy(g, 0, above)

    def down_copy(g):
        return row_copy(g, 1, below)

    def x_copy(t, tile, side):
        return remote(cen_raw.at[tile, side], cen_raw.at[t + 1, 0], x_send.at[t], x_recv.at[t], x_peer)

    def y_copy(t, tile, side):
        return remote(cen_raw.at[tile, side], cen_raw.at[t + 1, 1], y_send.at[t], y_recv.at[t], y_peer)

    def part_copy(j):
        zz, cc = member_at(j)
        return remote(
            part.at[2 * zz + cc], parts_in.at[j], part_send.at[j], part_recv.at[j], member(j)
        )

    def send_up(g):
        pl.when(up_ok)(lambda: up_copy(g).start())

    def send_down(g):
        pl.when(down_ok)(lambda: down_copy(g).start())

    send_up(2 * z + 1)
    send_down(2 * z)
    x_copy(1, 0, 0).start()
    y_copy(1, 1, 0).start()
    sib_copy(2 * z).start()
    sib_copy(2 * z + 1).start()
    send_up(2 * z)
    send_down(2 * z + 1)
    x_copy(2, 0, 1).start()
    y_copy(2, 1, 1).start()
    x_copy(3, 1, 0).start()
    y_copy(3, 0, 0).start()
    x_copy(4, 1, 1).start()
    y_copy(4, 0, 1).start()

    def ready_rows(g):
        emb_n[g, core] = unit_rows(emb_raw[g // 2, g % 2])

    def ready_sib(g):
        emb_n[g, 1 - core] = unit_rows(sib_raw[g // 2, g % 2])

    def ready_center(r):
        for side in range(2):
            cen_n[r, side] = unit_rows(cen_raw[r, side])

    def add_terms(g, first, last, others, targets):
        cosine = lax.dot_general(
            cen_n[first:last].reshape(-1, width),
            emb_n[g].reshape(2 * rows, width),
            (((1,), (1,)), ((), ())),
            preferred_element_type=jnp.float32,
        )
        label = jnp.concatenate([labels[g // 2, 0, g % 2], labels[g // 2, 1, g % 2]], axis=1)
        label = label - lax.broadcasted_iota(jnp.int32, (8, 2 * rows), 0)
        for m in range(2 * (last - first)):
            local = label - bases[2 * first + m]
            for q in range(0, quarter, 8):
                cos = cosine[m * quarter + q : m * quarter + q + 8]
                hit = local == q
                power = jnp.exp2(cos * (LOGIT_SCALE * math.log2(math.e)))
                others = others + jnp.where(hit, 0.0, power)
                targets = jnp.where(hit, cos, targets)
        return others, targets

    def pair(g, first, last):
        acc_o[g], acc_t[g] = add_terms(g, first, last, acc_o[g], acc_t[g])

    def blocks(lo, hi, first, last):
        @pl.loop(lo, hi)
        def _(zz):
            pair(2 * zz, first, last)
            pair(2 * zz + 1, first, last)

    for h in range(2):
        ready_rows(2 * z + h)
        ready_center(h)
    for h in range(2):
        sib_copy(2 * z + h).wait_recv()
        ready_sib(2 * z + h)
    blocks(z, z + 1, 0, 2)

    def receive_rows(t):
        low, high = 2 * z - t, 2 * z + 1 + t
        has_low, has_high = low >= 0, high < group

        @pl.when(has_low)
        def _():
            up_copy(low).wait_recv()
            sib_copy(low).start()
            send_up(low)

        @pl.when(has_high)
        def _():
            down_copy(high).wait_recv()
            sib_copy(high).start()
            send_down(high)

    def receive_centers(t):
        x_copy(t, 0, 0).wait_recv()
        y_copy(t, 0, 0).wait_recv()
        if t <= center_rounds - 4:
            x_copy(t + 4, t + 1, 1).start()
            y_copy(t + 4, t + 1, 0).start()

    def use_rows(t, tiles):
        low, high = 2 * z - t, 2 * z + 1 + t
        count = jnp.where(low >= 0, 1, 0) + jnp.where(high < group, 1, 0)

        @pl.loop(0, count)
        def _(i):
            g = jnp.where((low >= 0) & (i == 0), low, high)
            ready_rows(g)
            sib_copy(g).wait_recv()
            ready_sib(g)
            pair(g, 0, tiles)

    def span(t):
        return jnp.maximum(z - t // 2, 0), jnp.minimum(z + 1 + t // 2, depth)

    tiles = 2
    for t in range(1, min(rounds, center_rounds + 1)):
        receive_rows(t)
        receive_centers(t)
        ready_center(t + 1)
        if t == center_rounds - 1:
            blocks(*span(t - 1), tiles, t + 2)
            tiles = t + 2
        use_rows(t, tiles)
        if t % 2 == 0 and t < center_rounds:
            blocks(*span(t), tiles, t + 2)
            tiles = t + 2
    if rounds > center_rounds:

        @pl.loop(center_rounds + 1, rounds)
        def _(t):
            receive_rows(t)
            use_rows(t, tiles)

    receive_rows(rounds)
    if rounds == center_rounds:
        receive_centers(rounds)
        ready_center(rounds + 1)

    low_half = 2 * z < depth

    def give(g, sums):
        for quantity, total in enumerate(sums):
            total = jnp.sum(total, axis=0, keepdims=True)
            for cc in range(2):
                part[2 * (g // 2) + cc, quantity, g % 2] = total[:, cc * rows : (cc + 1) * rows]

    def send_parts(zz):
        step = lax.rem(zz + depth - z, depth)
        pl.when(step > 0)(lambda: part_copy(2 * step).start())
        part_copy(2 * step + 1).start()

    def place(j):
        return jnp.where(low_half, j, group - 1 - j)

    early = [place(j) for j in range(group - 1)]
    for first in range(0, group - 1, 7):
        some = early[first : first + 7]
        sums = [add_terms(g, tiles, center_tiles, acc_o[g], acc_t[g]) for g in some]
        for g, pair_sums in zip(some, sums):
            give(g, pair_sums)
    for i in range(depth - 1):
        send_parts(place(2 * i) // 2)

    final = place(group - 1)

    @pl.when(up_ok & down_ok)
    def _():
        give(final, add_terms(final, tiles, center_tiles, acc_o[final], acc_t[final]))

    @pl.when(jnp.logical_not(up_ok & down_ok))
    def _():
        ready_rows(final)
        sib_copy(final).wait_recv()
        ready_sib(final)
        give(final, add_terms(final, 0, center_tiles, acc_o[final], acc_t[final]))

    send_parts(final // 2)

    other_sum, target_cos = part[here, 0], part[here, 1]
    for j in range(1, group):
        part_copy(j).wait_recv()
        other_sum += parts_in[j, 0]
        target_cos += parts_in[j, 1]
    out_ref[...] = margin_loss(other_sum * math.exp(-LOGIT_SCALE), target_cos)

    for j in range(1, group):
        part_copy(j).wait_send()
    for t in range(1, center_rounds + 1):
        x_copy(t, 0, 0).wait_send()
        y_copy(t, 0, 0).wait_send()

    @pl.loop(0, group)
    def _(g):
        sib_copy(g).wait_send()
        pl.when(up_ok & (g < 2 * z + 2))(lambda: up_copy(g).wait_send())
        pl.when(down_ok & (g >= 2 * z))(lambda: down_copy(g).wait_send())


def body(depth, embeddings, centers, labels):
    count, width = embeddings.shape
    classes = centers.shape[0]
    rows, quarter, group, tiles = count // 2, classes // 4, 2 * depth, 8
    any_spec = pl.BlockSpec(memory_space=pltpu.HBM)
    dma = pltpu.SemaphoreType.DMA
    loss = pl.pallas_call(
        functools.partial(kernel, depth),
        out_shape=jax.ShapeDtypeStruct((2, 1, rows), jnp.float32),
        in_specs=[any_spec] * 3,
        out_specs=pl.BlockSpec(memory_space=pltpu.VMEM),
        scratch_shapes=[
            pltpu.VMEM((depth, 2, rows, width), jnp.bfloat16),
            pltpu.VMEM((depth, 2, rows, width), jnp.bfloat16),
            pltpu.VMEM((tiles, 2, quarter, width), jnp.bfloat16),
            pltpu.VMEM((group, 2, rows, width), jnp.bfloat16),
            pltpu.VMEM((tiles, 2, quarter, width), jnp.bfloat16),
            pltpu.VMEM((depth, 2, 2, 1, rows), jnp.int32),
            pltpu.VMEM((group, 8, 2 * rows), jnp.float32),
            pltpu.VMEM((group, 8, 2 * rows), jnp.float32),
            pltpu.VMEM((group, 2, 2, 1, rows), jnp.float32),
            pltpu.VMEM((group, 2, 2, 1, rows), jnp.float32),
            pltpu.SMEM((2 * tiles,), jnp.int32),
            dma((3,)),
            dma((3, group)),
            dma((2, group)),
            dma((3, group)),
            dma((2, group)),
            dma((tiles,)),
            dma((tiles,)),
            dma((tiles,)),
            dma((tiles,)),
            dma((group,)),
            dma((group,)),
        ],
        compiler_params=pltpu.CompilerParams(
            collective_id=0, has_side_effects=True, vmem_limit_bytes=60 * 1024 * 1024
        ),
    )(
        embeddings.reshape(2, rows, width),
        centers.reshape(2, 2, quarter, width),
        labels.reshape(2, 1, rows),
    )
    return loss.reshape(-1)


def solution(mesh):
    return jax.shard_map(
        functools.partial(body, mesh.shape["blk"] // 2),
        mesh=mesh,
        in_specs=(P(("dp", "blk"), None), P(("blk", "dp"), None), P(("dp", "blk"))),
        out_specs=P(("dp", "blk")),
        check_vma=False,
    )
```
